32 devices in a mesh: gx: 2 (over y), gy: 4 (over x, core), gz: 4 (over z).
Axes of the slice: x: 2, y: 2, z: 4, core: 2. Of those that a mesh axis runs over, the one named last changes fastest.
Arguments:
- halo_position: float32 [3, 16, 16, 8, 128], P(None, 'gx', 'gy', 'gz'), may hold values from 0 to 1
- halo_velocity: float32 [3, 16, 16, 8, 128], P(None, 'gx', 'gy', 'gz'), may hold values from -1 to 1
- halo_mass: float32 [16, 16, 8, 128], P('gx', 'gy', 'gz'), may hold values from 0.005 to 0.08
- cell_counts: int32 [16, 16, 8], P('gx', 'gy', 'gz'), may hold values from 1 to 128, as said below
Outputs:
- predicted: float32 [3, 16, 16, 8, 128], P(None, 'gx', 'gy', 'gz')
The draws below stay inside these ranges and needn't reach their ends.
Inputs may be any that keep to these rules, and one draw needn't show every extreme that they name: `cell_counts`: slots of a cell from its count on hold no halo.
All inputs are finite; a program needn't handle non-finite values.
Results may differ from the reference program's by a relative error of at most 0.0001.
Values sent between devices are 32-bit elements; how exact they have to be, the bound alone decides.
A program may use at most 64 MiB of HBM per device.

```python
import math
import jax
import jax.numpy as jnp
from jax import lax

CX = 8
CY = 4
CZ = 2
SLOTS = 128
NX = 16
NY = 16
NZ = 8


def draw_cell_counts(key, part):
    key_level, key_fill, key_peak = jax.random.split(key, 3)
    levels = jax.random.randint(key_level, (NX // CX, NY // CY, NZ // CZ), 0, 4)
    factor = jnp.left_shift(jnp.ones_like(levels), levels)
    factor = jnp.repeat(jnp.repeat(jnp.repeat(factor, CX, axis=0), CY, axis=1), CZ, axis=2)
    filled = jax.random.randint(key_fill, (NX, NY, NZ), 0, max(SLOTS // 4, 1))
    counts = jnp.minimum(1 + factor * filled, SLOTS)
    peak_cell = jax.random.randint(key_peak, (), 0, NX * NY * NZ)
    flattened = jnp.where(jnp.arange(NX * NY * NZ) == peak_cell, SLOTS, counts.reshape(-1))
    return flattened.reshape(NX, NY, NZ).astype(jnp.int32)


def steps_of(key, dims, cuts, least, top_value):
    def one(position, blocks):
        heights = jax.random.uniform(jax.random.fold_in(jax.random.fold_in(key, 6), position), (blocks,), jnp.float32, least / len(cuts), top_value / len(cuts))
        return jnp.repeat(jnp.exp(heights), dims[position] // blocks).reshape((-1,) + (1,) * (len(dims) - position - 1))

    loudness = one(*cuts[0])
    for cut in cuts[1:]:
        loudness = loudness * one(*cut)
    return loudness


def scatter_about(rng, extent, width, limit, cuts=(), kind=jnp.bfloat16):
    entries = width * jax.random.normal(rng, extent, jnp.float32)
    if cuts:
        entries = entries * steps_of(rng, extent, cuts, -0.22, 0.18)
    return jnp.clip(entries, -limit, limit).astype(kind)


def setup_inputs(seed: int = 0) -> dict:
    key_of = jax.random.split(jax.random.key(seed), 5)
    halo_position = jnp.clip(1.0 * jax.random.uniform(key_of[0], (3, NX, NY, NZ, SLOTS), jnp.float32) ** steps_of(key_of[0], (3, NX, NY, NZ, SLOTS), ((1, 2), (2, 4), (3, 4)), -0.2, 0.2), 0.0, 1.0)
    halo_velocity = scatter_about(key_of[1], (3, NX, NY, NZ, SLOTS), 0.2, 1.0, ((1, 2), (2, 4), (3, 4)), jnp.float32)
    halo_mass = jnp.clip(jnp.exp(math.log(0.08) - 2.7725887 * jax.random.uniform(key_of[2], (NX, NY, NZ, SLOTS), jnp.float32) ** steps_of(key_of[2], (NX, NY, NZ, SLOTS), ((0, 2), (1, 4), (2, 4)), -0.2, 0.2)), 0.005, 0.08)
    cell_counts = draw_cell_counts(jax.random.fold_in(key_of[4], 71), 0)
    return dict(halo_position=halo_position, halo_velocity=halo_velocity, halo_mass=halo_mass, cell_counts=cell_counts)


soft_sq = 0.01
cut_sq = 0.64

def pull_block(extended, targets):
    depth_x, depth_y, depth_z, slot_count = targets.shape[1:]
    anchor = jnp.int32(0)

    def add_offset(offset_code, running):
        offset_code = offset_code.astype(jnp.int32)
        shift_x = offset_code // 9
        shift_y = offset_code // 3 % 3
        shift_z = offset_code % 3
        sources = lax.dynamic_slice(extended, (anchor, shift_x, shift_y, shift_z, anchor), (4, depth_x, depth_y, depth_z, slot_count))
        delta_x = (sources[0] + (shift_x - 1).astype(jnp.float32))[..., :, None] - targets[0][..., None, :]
        delta_y = (sources[1] + (shift_y - 1).astype(jnp.float32))[..., :, None] - targets[1][..., None, :]
        delta_z = (sources[2] + (shift_z - 1).astype(jnp.float32))[..., :, None] - targets[2][..., None, :]
        dist_sq = delta_x * delta_x + delta_y * delta_y + delta_z * delta_z
        inv_dist = lax.rsqrt(dist_sq + soft_sq)
        tapering = jnp.maximum(1.0 - dist_sq / cut_sq, 0.0)
        weights = sources[3][..., :, None] * (inv_dist * inv_dist * inv_dist) * (tapering * tapering)
        return running + jnp.stack([lax.optimization_barrier(jnp.sum(weights * delta_x, axis=-2)), lax.optimization_barrier(jnp.sum(weights * delta_y, axis=-2)), lax.optimization_barrier(jnp.sum(weights * delta_z, axis=-2))], axis=0)
    return lax.fori_loop(jnp.int32(0), jnp.int32(27), add_offset, jnp.zeros(targets.shape, jnp.float32))

def pull_grid(field):
    padded = jnp.pad(field, ((0, 0), (1, 1), (1, 1), (1, 1), (0, 0)), mode='wrap')

    def one_plane(plane_index):
        window = lax.dynamic_slice_in_dim(padded, plane_index, 3, axis=1)
        targets = lax.dynamic_slice_in_dim(field[:3], plane_index, 1, axis=1)
        return pull_block(window, targets)[:, 0]
    planes = lax.map(one_plane, jnp.arange(field.shape[1], dtype=jnp.int32))
    return jnp.moveaxis(planes, 0, 1)

def reference(halo_position, halo_velocity, halo_mass, cell_counts):
    occupied = lax.broadcasted_iota(jnp.int32, halo_mass.shape, 3) < cell_counts[..., None]
    held_mass = jnp.where(occupied, halo_mass, 0.0)
    first_pull = pull_grid(jnp.concatenate([halo_position, held_mass[None]], axis=0))
    drifted = halo_position + halo_velocity + 0.5 * first_pull
    second_pull = pull_grid(jnp.concatenate([drifted, held_mass[None]], axis=0))
    predicted = halo_position + halo_velocity + first_pull / 3.0 + second_pull / 6.0
    return jnp.where(occupied[None], predicted, 0.0)
```

```python
import functools
import itertools

import jax
import jax.numpy as jnp
import numpy as np
from jax import lax
from jax.experimental import pallas as pl
from jax.experimental.pallas import tpu as pltpu
from jax.sharding import PartitionSpec as P

soft_sq = 0.01
cut_sq = 0.64
scale = 1.25
soft = soft_sq * scale * scale
top = 1.0 + soft
gain = scale**3 / scale
far = 8.0
K = 48


axes = ("gx", "gy", "gz")
MESH = pl.DeviceIdType.MESH


def exchange_kernel(dims, sizes, own, ext, send_sem, recv_sem):
    me = [lax.axis_index(a) for a in axes]
    moves = [o for o in itertools.product((-1, 0, 1), repeat=3) if any(o)]
    moves.sort(key=lambda o: -sum(map(abs, o)))

    def there(move):
        return tuple(lax.rem(m + o + n, n) for m, o, n in zip(me, move, sizes))

    barrier = pltpu.get_barrier_semaphore()
    for move in moves:
        pl.semaphore_signal(barrier, inc=1, device_id=there(move), device_id_type=MESH)
    pl.semaphore_wait(barrier, len(moves))
    copies = []
    for code, move in enumerate(moves):
        src = tuple(
            pl.ds(0, d) if o == 0 else pl.ds(d - 1 if o > 0 else 0, 1)
            for o, d in zip(move, dims)
        )
        dst = tuple(
            pl.ds(1, d) if o == 0 else pl.ds(0 if o > 0 else d + 1, 1)
            for o, d in zip(move, dims)
        )
        copy = pltpu.make_async_remote_copy(
            src_ref=own.at[src],
            dst_ref=ext.at[dst],
            send_sem=send_sem.at[code],
            recv_sem=recv_sem.at[code],
            device_id=there(move),
            device_id_type=MESH,
        )
        copy.start()
        copies.append(copy)
    for x in range(dims[0]):
        for y in range(dims[1]):
            ext[x + 1, y + 1, 1 : dims[2] + 1] = own[x, y]
    for copy in copies:
        copy.wait()


def exchange(own, collective_id):
    dims, sizes = own.shape[:3], [lax.axis_size(a) for a in axes]
    return pl.pallas_call(
        functools.partial(exchange_kernel, dims, sizes),
        out_shape=jax.ShapeDtypeStruct(tuple(d + 2 for d in dims) + own.shape[3:], jnp.float32),
        in_specs=[pl.BlockSpec(memory_space=pltpu.VMEM)],
        out_specs=pl.BlockSpec(memory_space=pltpu.VMEM),
        scratch_shapes=[pltpu.SemaphoreType.DMA((26,)), pltpu.SemaphoreType.DMA((26,))],
        compiler_params=pltpu.CompilerParams(
            collective_id=collective_id, has_side_effects=True, vmem_limit_bytes=8 * 2**20
        ),
        name="exchange",
    )(own)


def parts_of(value):
    first = value.astype(jnp.bfloat16).astype(jnp.float32)
    rest = value - first
    second = rest.astype(jnp.bfloat16).astype(jnp.float32)
    third = (rest - second).astype(jnp.bfloat16).astype(jnp.float32)
    return first, second, third


def shift_tables():
    shifts = np.array(list(itertools.product((-1, 0, 1), repeat=3)), np.float32)
    offs = np.zeros((3, 32, 1), np.float32)
    offs[:, :27, 0] = scale * shifts.T
    offs = np.broadcast_to(offs, (3, 32, 128))
    rows = np.zeros((32, 16, 1), np.float32)
    for c in range(3):
        rows[:27, 3 + 3 * c : 6 + 3 * c, 0] = 2 * scale * shifts[:, c, None]
    return jnp.asarray(offs), jnp.asarray(np.broadcast_to(rows, (32, 16, 128)))


def pull_kernel(dims, width, last, src, base_in, offs, rows, *refs):
    if last:
        (out, a_scr, r_scr, t_scr, v_scr, row_scr, m_scr, w_scr), drift = refs, None
    else:
        out, drift, a_scr, r_scr, t_scr, v_scr, row_scr, m_scr, w_scr = refs
    pull_cells(dims, width, src, base_in, offs, rows, out, drift, a_scr, r_scr, t_scr, v_scr, row_scr, m_scr, w_scr)


def pull_cells(dims, width, src, base_in, offs, rows, out, drift, a_scr, r_scr, t_scr, v_scr, row_scr, m_scr, w_scr):
    dx, dy, dz = dims
    ey, ez = dy + 2, dz + 2
    cells = (dx + 2) * ey * ez
    ones = jnp.ones((8, 128), jnp.float32)
    zeros = jnp.zeros((8, 128), jnp.float32)
    for n in range(v_scr.shape[0]):
        v_scr[n] = rows[...]
    row_scr[...] = jnp.zeros(row_scr.shape, jnp.float32)
    m_scr[...] = jnp.zeros(m_scr.shape, jnp.float32)
    w_scr[...] = jnp.zeros(w_scr.shape, jnp.float32)
    for k in range(3):
        row_scr[:, 32 + k, :] = ones
        w_scr[:, 18 + k, :] = ones

    @pl.loop(0, cells // 8, unroll=2)
    def _(group):
        base = pl.multiple_of(group * 8, 8)
        mass = src[pl.ds(base * 4 + 3, 8, stride=4), :]
        a = [(src[pl.ds(base * 4 + c, 8, stride=4), :] - 0.5) * scale for c in range(3)]
        a = [jnp.where(mass > 0.0, v, 0.0) for v in a]
        split = [parts_of(v) for v in a]
        norm = parts_of(a[0] * a[0] + a[1] * a[1] + a[2] * a[2])
        left = []
        for p in split:
            left += [p[0], p[0], p[1], p[0], p[2], p[1]]
        left += list(norm) + [None] * 14
        for p in split:
            left += list(p)
        for k, v in enumerate(left):
            if v is not None:
                row_scr[:, k, :] = v
        right = []
        for c in range(3):
            p = parts_of(a[c] * -2.0)
            right += [p[0], p[1], p[0], p[2], p[0], p[1]]
        mm = [parts_of(mass * v) for v in a] + [parts_of(mass)]
        order = list(mm[0]) + list(mm[1]) + [None] * 2 + list(mm[2]) + list(mm[3])
        for k, v in enumerate(order):
            if v is not None:
                m_scr[:, k, :] = v
        for j in range(8):
            a_scr[base + j] = row_scr[j].T.astype(jnp.bfloat16)
            r = m_scr[j].astype(jnp.bfloat16)
            r_scr[base + j] = jnp.concatenate([r, r], axis=1)
        for k, v in enumerate(right):
            w_scr[:, k, :] = v
        for j in range(8):
            t_scr[base + j] = w_scr[j].astype(jnp.bfloat16)

    def near(i, v_scr):
        x = i // (dy * dz)
        y = i // dz % dy
        z = i % dz
        me = ((x + 1) * ey + y + 1) * ez + z + 1
        held = src[pl.ds(me * 4 + 3, 1), :] > 0.0
        t = [jnp.where(held, (src[pl.ds(me * 4 + c, 1), :] - 0.5) * scale, 0.0) for c in range(3)]
        norm = soft
        for c in range(3):
            d = t[c] - offs[c]
            norm = norm + d * d
        for k, v in enumerate(parts_of(norm)):
            v_scr[:, k, :] = v
        fixed = t_scr[me]
        reach = jnp.max(jnp.maximum(jnp.maximum(jnp.abs(t[0]), jnp.abs(t[1])), jnp.abs(t[2])))

        acc = jnp.zeros((16, 128), jnp.float32)
        leans = [zeros, zeros, zeros]
        for code, shift in enumerate(itertools.product(range(3), repeat=3)):
            other = ((x + shift[0]) * ey + y + shift[1]) * ez + z + shift[2]
            right = jnp.concatenate([fixed, v_scr[code].astype(jnp.bfloat16)], axis=0)
            v = jnp.dot(a_scr[other], right, preferred_element_type=jnp.float32)
            r = lax.rsqrt(v)
            g = r * jnp.maximum(top - v, 0.0)
            w = g * g * r
            hi = w.astype(jnp.bfloat16)
            lo = (w - hi.astype(jnp.float32)).astype(jnp.bfloat16)
            f = jnp.dot(
                r_scr[other],
                jnp.concatenate([hi, lo], axis=0),
                preferred_element_type=jnp.float32,
            )
            acc = acc + f
            for c in range(3):
                if shift[c] != 1:
                    leans[c] = leans[c] + f[8:] * float(shift[c] - 1)

        def three(v, k):
            return v[k : k + 1] + v[k + 1 : k + 2] + v[k + 2 : k + 3]

        m = three(acc, 11)
        for c, k in enumerate((0, 3, 8)):
            finish(i, me, c, gain * (three(acc, k) + scale * three(leans[c], 3) - t[c] * m))
        if drift is not None:
            drift[pl.ds(i * 4 + 3, 1), :] = src[pl.ds(me * 4 + 3, 1), :]
        return reach

    def finish(i, me, c, pull):
        if drift is None:
            held = src[pl.ds(me * 4 + 3, 1), :] > 0.0
            out[c, pl.ds(i, 1), :] = jnp.where(held, base_in[c, pl.ds(i, 1), :] + pull * (1 / 6), 0.0)
        else:
            moved = src[pl.ds(me * 4 + c, 1), :] + base_in[c, pl.ds(i, 1), :]
            out[c, pl.ds(i, 1), :] = moved + pull * (1 / 3)
            drift[pl.ds(i * 4 + c, 1), :] = moved + 0.5 * pull

    def afar(i, reach):
        x = i // (dy * dz)
        y = i // dz % dy
        z = i % dz
        me = ((x + 1) * ey + y + 1) * ez + z + 1

        @pl.when(reach > far)
        def _():
            def one(code, carry):
                sx, sy, sz = code // 9, code // 3 % 3, code % 3
                other = ((x + sx) * ey + y + sy) * ez + z + sz
                for k in range(4):
                    w_scr[0, k : k + 1, :] = src[pl.ds(other * 4 + k, 1), :]
                cols = w_scr[0, :8].T
                deltas = []
                q = 0.0
                for c, s in enumerate((sx, sy, sz)):
                    d = cols[:, c : c + 1] + (s - 1).astype(jnp.float32) - src[pl.ds(me * 4 + c, 1), :]
                    deltas.append(d)
                    q = q + d * d
                r = lax.rsqrt(q + soft_sq)
                taper = jnp.maximum(1.0 - q * (1.0 / cut_sq), 0.0)
                w = cols[:, 3:4] * (r * r * r) * (taper * taper)
                return tuple(
                    v + jnp.sum(w * d, axis=0, keepdims=True) for v, d in zip(carry, deltas)
                )

            zero = jnp.zeros((1, 128), jnp.float32)
            pulls = lax.fori_loop(0, 27, one, (zero, zero, zero))
            for c in range(3):
                finish(i, me, c, pulls[c])

    @pl.loop(0, dx * dy * dz // width)
    def _(step):
        reaches = [near(step * width + n, v_scr.at[n]) for n in range(width)]
        for n in range(width):
            afar(step * width + n, reaches[n])


def pull_field(extended, base_in, last):
    ex, ey, ez, comps, slots = extended.shape
    dims = (ex - 2, ey - 2, ez - 2)
    cells = ex * ey * ez
    offs, rows = shift_tables()
    own = dims[0] * dims[1] * dims[2]
    width = 4 if own % 4 == 0 else 1
    field = jax.ShapeDtypeStruct((3, own, slots), jnp.float32)
    drift = jax.ShapeDtypeStruct((own * comps, slots), jnp.float32)
    vmem = pl.BlockSpec(memory_space=pltpu.VMEM)
    return pl.pallas_call(
        functools.partial(pull_kernel, dims, width, last),
        out_shape=field if last else (field, drift),
        in_specs=[vmem] * 4,
        out_specs=vmem if last else (vmem, vmem),
        scratch_shapes=[
            pltpu.VMEM((cells, slots, K), jnp.bfloat16),
            pltpu.VMEM((cells, 16, 2 * slots), jnp.bfloat16),
            pltpu.VMEM((cells, 32, slots), jnp.bfloat16),
            pltpu.VMEM((width, 32, 16, slots), jnp.float32),
            pltpu.VMEM((8, K, slots), jnp.float32),
            pltpu.VMEM((8, 16, slots), jnp.float32),
            pltpu.VMEM((8, 32, slots), jnp.float32),
        ],
        compiler_params=pltpu.CompilerParams(vmem_limit_bytes=48 * 2**20),
        name="pulls",
    )(extended.reshape(cells * comps, slots), base_in, offs, rows)


def body(halo_position, halo_velocity, halo_mass, cell_counts):
    dims, slots = halo_mass.shape[:3], halo_mass.shape[3]
    occupied = lax.broadcasted_iota(jnp.int32, halo_mass.shape, 3) < cell_counts[..., None]
    held_mass = jnp.where(occupied, halo_mass, 0.0)
    outgoing = jnp.concatenate([jnp.moveaxis(halo_position, 0, 3), held_mass[..., None, :]], axis=3)
    velocity = halo_velocity.reshape(3, -1, slots)
    part, drift = pull_field(exchange(outgoing, 0), velocity, False)
    predicted = pull_field(exchange(drift.reshape(outgoing.shape), 1), part, True)
    return predicted.reshape(halo_position.shape)


def solution(mesh):
    return jax.shard_map(
        body,
        mesh=mesh,
        in_specs=(
            P(None, "gx", "gy", "gz", None),
            P(None, "gx", "gy", "gz", None),
            P("gx", "gy", "gz", None),
            P("gx", "gy", "gz"),
        ),
        out_specs=P(None, "gx", "gy", "gz", None),
        check_vma=False,
    )
```

```python
import functools
import itertools

import jax
import jax.numpy as jnp
import numpy as np
from jax import lax
from jax.experimental import pallas as pl
from jax.experimental.pallas import tpu as pltpu
from jax.sharding import PartitionSpec as P

soft_sq = 0.01
cut_sq = 0.64
scale = 1.25
soft = soft_sq * scale * scale
top = 1.0 + soft
gain = scale**3 / scale
far = 8.0
K = 48


axes = ("gx", "gy", "gz")
MESH = pl.DeviceIdType.MESH
moves = sorted((o for o in itertools.product((-1, 0, 1), repeat=3) if any(o)), key=lambda o: -sum(map(abs, o)))
shifts = list(itertools.product(range(3), repeat=3))


def parts_of(value):
    first = value.astype(jnp.bfloat16).astype(jnp.float32)
    rest = value - first
    second = rest.astype(jnp.bfloat16).astype(jnp.float32)
    third = (rest - second).astype(jnp.bfloat16).astype(jnp.float32)
    return first, second, third


def shift_tables():
    shifts = np.array(list(itertools.product((-1, 0, 1), repeat=3)), np.float32)
    offs = np.zeros((3, 32, 1), np.float32)
    offs[:, :27, 0] = scale * shifts.T
    offs = np.broadcast_to(offs, (3, 32, 128))
    rows = np.zeros((32, 16, 1), np.float32)
    for c in range(3):
        rows[:27, 3 + 3 * c : 6 + 3 * c, 0] = 2 * scale * shifts[:, c, None]
    return jnp.asarray(offs), jnp.asarray(np.broadcast_to(rows, (32, 16, 128)))


def there(sizes, move):
    return tuple(lax.rem(lax.axis_index(a) + o + n, n) for a, o, n in zip(axes, move, sizes))


def halo_copies(dims, sizes, own, halo_x, halo_y, halo_z, send_sem, recv_sem):
    def leaving(o, d):
        return pl.ds(0, d) if o == 0 else pl.ds(d - 1 if o > 0 else 0, 1)

    def landing(o, d):
        return pl.ds(1, d) if o == 0 else pl.ds(0 if o > 0 else d + 1, 1)

    copies = []
    for code, move in enumerate(moves):
        ox, oy, oz = move
        side = [0 if o > 0 else 1 for o in move]
        edge = [d - 1 if o > 0 else 0 for o, d in zip(move, dims)]
        ys, zs = leaving(oy, dims[1]), leaving(oz, dims[2])
        if ox:
            src = own.at[edge[0], ys, zs]
            dst = halo_x.at[side[0], landing(oy, dims[1]), landing(oz, dims[2])]
        elif oy:
            src = own.at[:, edge[1], zs]
            dst = halo_y.at[:, side[1], landing(oz, dims[2])]
        else:
            src = own.at[:, :, edge[2]]
            dst = halo_z.at[:, side[2]]
        copies.append(
            pltpu.make_async_remote_copy(
                src_ref=src,
                dst_ref=dst,
                send_sem=send_sem.at[code],
                recv_sem=recv_sem.at[code],
                device_id=there(sizes, move),
                device_id_type=MESH,
            )
        )
    return copies


def pull_kernel(dims, sizes, last, own, base_in, offs, rows, *refs):
    if last:
        out, reach, halo_x, halo_y, halo_z, *scratch = refs
        drift = None
    else:
        out, drift, halo_x, halo_y, halo_z, *scratch = refs
    a_scr, r_scr, t_scr, v_scr, p_scr, row_scr, m_scr, w_scr, send_sem, recv_sem = scratch
    dx, dy, dz = dims
    ex, ey, ez = dx + 2, dy + 2, dz + 2
    barrier = pltpu.get_barrier_semaphore()
    for move in moves:
        pl.semaphore_signal(barrier, inc=1, device_id=there(sizes, move), device_id_type=MESH)

    zeros = jnp.zeros((8, 128), jnp.float32)

    @pl.loop(0, dx * dy * dz, unroll=2)
    def _(n):
        v_scr[n] = rows[...]

    row_scr[...] = jnp.zeros(row_scr.shape, jnp.float32)
    m_scr[...] = jnp.zeros(m_scr.shape, jnp.float32)
    w_scr[...] = jnp.zeros(w_scr.shape, jnp.float32)
    for k in range(3):
        row_scr[:, 32 + k, :] = jnp.ones((16, 128), jnp.float32)
        w_scr[:, 18 + k, :] = jnp.ones((8, 128), jnp.float32)

    def prepare(cells, place, slot, targets):
        cells = cells.reshape(8, 4, 128)
        mass = cells[:, 3, :]
        a = [(cells[:, c, :] - 0.5) * scale for c in range(3)]
        a = [jnp.where(mass > 0.0, v, 0.0) for v in a]
        split = [parts_of(v) for v in a]
        norm = parts_of(a[0] * a[0] + a[1] * a[1] + a[2] * a[2])
        left = []
        for p in split:
            left += [p[0], p[0], p[1], p[0], p[2], p[1]]
        left += list(norm) + [None] * 14
        for p in split:
            left += list(p)
        for k, v in enumerate(left):
            if v is not None:
                row_scr[slot : slot + 8, k, :] = v
        mm = [parts_of(mass * v) for v in a] + [parts_of(mass)]
        order = list(mm[0]) + list(mm[1]) + [None] * 2 + list(mm[2]) + list(mm[3])
        for k, v in enumerate(order):
            if v is not None:
                m_scr[slot : slot + 8, k, :] = v
        for j in range(8):
            a_scr[place(j)] = row_scr[slot + j].T.astype(jnp.bfloat16)
            r = m_scr[slot + j].astype(jnp.bfloat16)
            r_scr[place(j)] = jnp.concatenate([r, r], axis=1)
        if targets is not None:
            right = []
            for c in range(3):
                p = parts_of(a[c] * -2.0)
                right += [p[0], p[1], p[0], p[2], p[0], p[1]]
            for k, v in enumerate(right):
                w_scr[:, k, :] = v
            for j in range(8):
                t_scr[targets + j] = w_scr[j].astype(jnp.bfloat16)

    @pl.loop(0, dx)
    def _(x):
        prepare(own[x], lambda j: ((x + 1) * ey + j // dz + 1) * ez + j % dz + 1, 0, x * dy * dz)

    pl.semaphore_wait(barrier, len(moves))
    copies = halo_copies(dims, sizes, own, halo_x, halo_y, halo_z, send_sem, recv_sem)
    for copy in copies:
        copy.start()

    def point(x, y, z):
        cell = own[x, y, z]
        held = cell[3:] > 0.0
        return [jnp.where(held, (cell[c : c + 1] - 0.5) * scale, 0.0) for c in range(3)]

    def norms(x, y, z):
        i = (x * dy + y) * dz + z
        t = point(x, y, z)
        norm = soft
        for c in range(3):
            d = t[c] - offs[c]
            norm = norm + d * d
        for k, v in enumerate(parts_of(norm)):
            v_scr[i, :, k, :] = v
        if last:
            reach[pl.ds(i, 1), :] = jnp.maximum(jnp.maximum(jnp.abs(t[0]), jnp.abs(t[1])), jnp.abs(t[2]))

    def gather(x, y, z, codes, acc, leans):
        i = (x * dy + y) * dz + z
        fixed = t_scr[i]
        for shift in codes:
            code = shifts.index(shift)
            other = ((x + shift[0]) * ey + y + shift[1]) * ez + z + shift[2]
            right = jnp.concatenate([fixed, v_scr[i, code].astype(jnp.bfloat16)], axis=0)
            v = jnp.dot(a_scr[other], right, preferred_element_type=jnp.float32)
            r = lax.rsqrt(v)
            g = r * jnp.maximum(top - v, 0.0)
            w = g * g * r
            hi = w.astype(jnp.bfloat16)
            lo = (w - hi.astype(jnp.float32)).astype(jnp.bfloat16)
            f = jnp.dot(
                r_scr[other],
                jnp.concatenate([hi, lo], axis=0),
                preferred_element_type=jnp.float32,
            )
            acc = acc + f
            for c in range(3):
                if shift[c] != 1:
                    leans[c] = leans[c] + f[8:] * float(shift[c] - 1)
        return acc, leans

    def early(shift, x, z):
        return shift[1] == 1 and 0 <= x + shift[0] - 1 < dx and 0 <= z + shift[2] - 1 < dz

    @pl.loop(0, dy)
    def _(y):
        for x in range(dx):
            for z in range(dz):
                norms(x, y, z)
                codes = [s for s in shifts if early(s, x, z)]
                acc, leans = gather(x, y, z, codes, jnp.zeros((16, 128), jnp.float32), [zeros] * 3)
                i = (x * dy + y) * dz + z
                p_scr[i, :16] = acc
                p_scr[i, 16:24] = leans[0]
                p_scr[i, 24:] = leans[2]

    for copy in copies:
        copy.wait()

    per = 8 // ez

    @pl.loop(0, 2 * (ey // per))
    def _(g):
        side, q = g // (ey // per), g % (ey // per)
        cells = halo_x[side, pl.ds(q * per, per)]
        prepare(cells, lambda j: (side * (ex - 1) * ey + q * per + j // ez) * ez + j % ez, 0, None)

    @pl.loop(0, dx)
    def _(x):
        prepare(halo_y[x], lambda j: ((x + 1) * ey + j // ez * (ey - 1)) * ez + j % ez, 0, None)
        prepare(halo_z[x], lambda j: ((x + 1) * ey + j % dy + 1) * ez + j // dy * (ez - 1), 8, None)

    def three(v, k):
        return v[k : k + 1] + v[k + 1 : k + 2] + v[k + 2 : k + 3]

    def finish(x, y, z, like):
        i = (x * dy + y) * dz + z
        codes = [s for s in shifts if not early(s, like, z)]
        acc, leans = gather(x, y, z, codes, p_scr[i, :16], [p_scr[i, 16:24], zeros, p_scr[i, 24:]])
        t = point(x, y, z)
        m = three(acc, 11)
        cell = own[x, y, z]
        for c, k in enumerate((0, 3, 8)):
            pull = gain * (three(acc, k) + scale * three(leans[c], 3) - t[c] * m)
            if last:
                out[c, pl.ds(i, 1), :] = jnp.where(cell[3:] > 0.0, base_in[c, pl.ds(i, 1), :] + pull * (1 / 6), 0.0)
            else:
                moved = cell[c : c + 1] + base_in[c, pl.ds(i, 1), :]
                out[c, pl.ds(i, 1), :] = moved + pull * (1 / 3)
                drift[x, y, z, c : c + 1, :] = moved + 0.5 * pull
        if not last:
            drift[x, y, z, 3:, :] = cell[3:]

    wide = 2 if (dx - 2) % 2 == 0 else 1

    @pl.loop(0, (dx - 2) // wide * dy)
    def _(step):
        for n in range(wide):
            for z in range(dz):
                finish(1 + step // dy * wide + n, step % dy, z, 1)

    @pl.loop(0, dy)
    def _(y):
        for x in (0, dx - 1):
            for z in range(dz):
                finish(x, y, z, x)


def pull_field(cells, base_in, last):
    dx, dy, dz, comps, slots = cells.shape
    dims, sizes = (dx, dy, dz), [lax.axis_size(a) for a in axes]
    own, every = dx * dy * dz, (dx + 2) * (dy + 2) * (dz + 2)
    offs, rows = shift_tables()
    field = jax.ShapeDtypeStruct((3, own, slots), jnp.float32)
    second = jax.ShapeDtypeStruct((own, slots) if last else cells.shape, jnp.float32)
    halos = [
        jax.ShapeDtypeStruct(s + (comps, slots), jnp.float32)
        for s in ((2, dy + 2, dz + 2), (dx, 2, dz + 2), (dx, 2, dy))
    ]
    vmem = pl.BlockSpec(memory_space=pltpu.VMEM)
    return pl.pallas_call(
        functools.partial(pull_kernel, dims, sizes, last),
        out_shape=[field, second] + halos,
        in_specs=[vmem] * 4,
        out_specs=[vmem] * 5,
        scratch_shapes=[
            pltpu.VMEM((every, slots, K), jnp.bfloat16),
            pltpu.VMEM((every, 16, 2 * slots), jnp.bfloat16),
            pltpu.VMEM((own, 32, slots), jnp.bfloat16),
            pltpu.VMEM((own, 32, 16, slots), jnp.float32),
            pltpu.VMEM((own, 32, slots), jnp.float32),
            pltpu.VMEM((16, K, slots), jnp.float32),
            pltpu.VMEM((16, 16, slots), jnp.float32),
            pltpu.VMEM((8, 32, slots), jnp.float32),
            pltpu.SemaphoreType.DMA((len(moves),)),
            pltpu.SemaphoreType.DMA((len(moves),)),
        ],
        compiler_params=pltpu.CompilerParams(
            collective_id=int(last),
            has_side_effects=True,
            vmem_limit_bytes=52 * 2**20,
        ),
        name="pulls",
    )(cells, base_in, offs, rows)


def far_kernel(dims, src, part, near, out, w_scr):
    dx, dy, dz = dims
    ey, ez = dy + 2, dz + 2
    out[...] = near[...]

    @pl.loop(0, dx * dy * dz)
    def _(i):
        x, y, z = i // (dy * dz), i // dz % dy, i % dz
        me = src[((x + 1) * ey + y + 1) * ez + z + 1]
        held = me[3:] > 0.0
        t = [jnp.where(held, jnp.abs(me[c : c + 1] - 0.5) * scale, 0.0) for c in range(3)]

        @pl.when(jnp.max(jnp.maximum(jnp.maximum(t[0], t[1]), t[2])) > far)
        def _():
            def one(code, carry):
                sx, sy, sz = code // 9, code // 3 % 3, code % 3
                w_scr[:4, :] = src[((x + sx) * ey + y + sy) * ez + z + sz]
                cols = w_scr[...].T
                deltas = []
                q = 0.0
                for c, s in enumerate((sx, sy, sz)):
                    d = cols[:, c : c + 1] + (s - 1).astype(jnp.float32) - me[c : c + 1]
                    deltas.append(d)
                    q = q + d * d
                r = lax.rsqrt(q + soft_sq)
                taper = jnp.maximum(1.0 - q * (1.0 / cut_sq), 0.0)
                w = cols[:, 3:4] * (r * r * r) * (taper * taper)
                return tuple(
                    v + jnp.sum(w * d, axis=0, keepdims=True) for v, d in zip(carry, deltas)
                )

            zero = jnp.zeros((1, 128), jnp.float32)
            pulls = lax.fori_loop(0, 27, one, (zero, zero, zero))
            for c in range(3):
                out[c, pl.ds(i, 1), :] = jnp.where(held, part[c, pl.ds(i, 1), :] + pulls[c] * (1 / 6), 0.0)


def far_field(cells, part, near, halo_x, halo_y, halo_z):
    dx, dy, dz, comps, slots = cells.shape
    ring = jnp.moveaxis(halo_z, 1, 2)
    inner = jnp.concatenate([ring[:, :, :1], cells, ring[:, :, 1:]], axis=2)
    inner = jnp.concatenate([halo_y[:, :1], inner, halo_y[:, 1:]], axis=1)
    every = jnp.concatenate([halo_x[:1], inner, halo_x[1:]], axis=0)
    vmem = pl.BlockSpec(memory_space=pltpu.VMEM)
    return pl.pallas_call(
        functools.partial(far_kernel, (dx, dy, dz)),
        out_shape=jax.ShapeDtypeStruct(near.shape, jnp.float32),
        in_specs=[vmem] * 3,
        out_specs=vmem,
        scratch_shapes=[pltpu.VMEM((8, slots), jnp.float32)],
        name="far_pulls",
    )(every.reshape(-1, comps, slots), part, near)


def body(halo_position, halo_velocity, halo_mass, cell_counts):
    slots = halo_mass.shape[3]
    occupied = lax.broadcasted_iota(jnp.int32, halo_mass.shape, 3) < cell_counts[..., None]
    held_mass = jnp.where(occupied, halo_mass, 0.0)
    cells = jnp.concatenate([jnp.moveaxis(halo_position, 0, 3), held_mass[..., None, :]], axis=3)
    part, drift = pull_field(cells, halo_velocity.reshape(3, -1, slots), False)[:2]
    near, reach, *halos = pull_field(drift, part, True)
    predicted = lax.cond(
        jnp.max(reach) > far,
        lambda: far_field(drift, part, near, *halos),
        lambda: near,
    )
    return predicted.reshape(halo_position.shape)


def solution(mesh):
    return jax.shard_map(
        body,
        mesh=mesh,
        in_specs=(
            P(None, "gx", "gy", "gz", None),
            P(None, "gx", "gy", "gz", None),
            P("gx", "gy", "gz", None),
            P("gx", "gy", "gz"),
        ),
        out_specs=P(None, "gx", "gy", "gz", None),
        check_vma=False,
    )
```

```python
import functools
import itertools

import jax
import jax.numpy as jnp
from jax import lax
from jax.experimental import pallas as pl
from jax.experimental.pallas import tpu as pltpu
from jax.sharding import PartitionSpec as P

soft_sq = 0.01
cut_sq = 0.64
scale = 1.25
soft = soft_sq * scale * scale
top = 1.0 + soft
gain = scale**3 / scale
far = 8.0
K = 48


axes = ("gx", "gy", "gz")
MESH = pl.DeviceIdType.MESH
moves = sorted((o for o in itertools.product((-1, 0, 1), repeat=3) if any(o)), key=lambda o: -sum(map(abs, o)))
shifts = sorted(itertools.product(range(3), repeat=3), key=lambda s: s[1] != 1)


def parts_of(value):
    first = value.astype(jnp.bfloat16).astype(jnp.float32)
    rest = value - first
    second = rest.astype(jnp.bfloat16).astype(jnp.float32)
    third = (rest - second).astype(jnp.bfloat16).astype(jnp.float32)
    return first, second, third


def there(sizes, move):
    return tuple(lax.rem(lax.axis_index(a) + o + n, n) for a, o, n in zip(axes, move, sizes))


def halo_copies(dims, sizes, own, halo_x, halo_y, halo_z, send_sem, recv_sem):
    def leaving(o, d):
        return pl.ds(0, d) if o == 0 else pl.ds(d - 1 if o > 0 else 0, 1)

    def landing(o, d):
        return pl.ds(1, d) if o == 0 else pl.ds(0 if o > 0 else d + 1, 1)

    copies = []
    for code, move in enumerate(moves):
        ox, oy, oz = move
        side = [0 if o > 0 else 1 for o in move]
        edge = [d - 1 if o > 0 else 0 for o, d in zip(move, dims)]
        ys, zs = leaving(oy, dims[1]), leaving(oz, dims[2])
        if ox:
            src = own.at[edge[0], ys, zs]
            dst = halo_x.at[side[0], landing(oy, dims[1]), landing(oz, dims[2])]
        elif oy:
            src = own.at[:, edge[1], zs]
            dst = halo_y.at[:, side[1], landing(oz, dims[2])]
        else:
            src = own.at[:, :, edge[2]]
            dst = halo_z.at[:, side[2]]
        copies.append(
            pltpu.make_async_remote_copy(
                src_ref=src,
                dst_ref=dst,
                send_sem=send_sem.at[code],
                recv_sem=recv_sem.at[code],
                device_id=there(sizes, move),
                device_id_type=MESH,
            )
        )
    return copies


def pull_kernel(dims, sizes, last, own, base_in, *refs):
    if last:
        out, reach, halo_x, halo_y, halo_z, *scratch = refs
        drift = None
    else:
        out, drift, halo_x, halo_y, halo_z, *scratch = refs
    a_scr, r_scr, t_scr, v_scr, p_scr, offs, raw_scr, row_scr, m_scr, w_scr, send_sem, recv_sem = scratch
    dx, dy, dz = dims
    ex, ey, ez = dx + 2, dy + 2, dz + 2
    barrier = pltpu.get_barrier_semaphore()
    for move in moves:
        pl.semaphore_signal(barrier, inc=1, device_id=there(sizes, move), device_id_type=MESH)

    zeros = jnp.zeros((8, 128), jnp.float32)
    for code, shift in enumerate(shifts):
        for c in range(3):
            offs[c, code : code + 1, :] = jnp.full((1, 128), scale * (shift[c] - 1), jnp.float32)
    for c in range(3):
        offs[c, 27:, :] = jnp.zeros((5, 128), jnp.float32)

    @pl.loop(0, v_scr.shape[0])
    def _(n):
        v_scr[n] = jnp.zeros(v_scr.shape[1:], jnp.float32)
        for c in range(3):
            for k in range(3 + 3 * c, 6 + 3 * c):
                for block in range(4):
                    v_scr[n, block, 8 * k : 8 * k + 8, :] = 2 * offs[c, 8 * block : 8 * block + 8]

    row_scr[...] = jnp.zeros(row_scr.shape, jnp.float32)
    m_scr[...] = jnp.zeros(m_scr.shape, jnp.float32)
    w_scr[...] = jnp.zeros(w_scr.shape, jnp.float32)
    row_scr[:, 256:280, :] = jnp.ones((2, 24, 128), jnp.float32)
    w_scr[:, 144:168, :] = jnp.ones((2, 24, 128), jnp.float32)

    def prepare(cells, place, slot, targets):
        cells = cells.reshape(8, 4, 128)
        for j in range(8):
            raw_scr[slot, 4 * j : 4 * j + 4, :] = cells[j]
        mass = raw_scr[slot, pl.ds(3, 8, stride=4), :]
        a = [(raw_scr[slot, pl.ds(c, 8, stride=4), :] - 0.5) * scale for c in range(3)]
        a = [jnp.where(mass > 0.0, v, 0.0) for v in a]
        split = [parts_of(v) for v in a]
        norm = parts_of(a[0] * a[0] + a[1] * a[1] + a[2] * a[2])
        left = []
        for p in split:
            left += [p[0], p[0], p[1], p[0], p[2], p[1]]
        left += list(norm) + [None] * 14
        for p in split:
            left += list(p)
        for k, v in enumerate(left):
            if v is not None:
                row_scr[slot, 8 * k : 8 * k + 8, :] = v
        mm = [parts_of(mass * v) for v in a] + [parts_of(mass)]
        order = list(mm[0]) + list(mm[1]) + [None] * 2 + list(mm[2]) + list(mm[3])
        for k, v in enumerate(order):
            if v is not None:
                m_scr[slot, 8 * k : 8 * k + 8, :] = v
        for j in range(8):
            a_scr[place(j)] = row_scr[slot, pl.ds(j, K, stride=8), :].T.astype(jnp.bfloat16)
            r = m_scr[slot, pl.ds(j, 16, stride=8), :].astype(jnp.bfloat16)
            r_scr[place(j)] = jnp.concatenate([r, r], axis=1)
        if targets is not None:
            right = []
            for c in range(3):
                p = parts_of(a[c] * -2.0)
                right += [p[0], p[1], p[0], p[2], p[0], p[1]]
            for k, v in enumerate(right):
                w_scr[slot, 8 * k : 8 * k + 8, :] = v
            for j in range(8):
                t_scr[targets + j] = w_scr[slot, pl.ds(j, 32, stride=8), :].astype(jnp.bfloat16)

    def prepare_own(x, slot):
        prepare(own[x], lambda j: ((x + 1) * ey + j // dz + 1) * ez + j % dz + 1, slot, x * dy * dz)

    pair = 2 if dx % 2 == 0 else 1

    @pl.loop(0, dx // pair)
    def _(half):
        for n in range(pair):
            prepare_own(half * pair + n, n)

    pl.semaphore_wait(barrier, len(moves))
    copies = halo_copies(dims, sizes, own, halo_x, halo_y, halo_z, send_sem, recv_sem)
    for copy in copies:
        copy.start()

    def point(x, y, z):
        cell = own[x, y, z]
        held = cell[3:] > 0.0
        return [jnp.where(held, (cell[c : c + 1] - 0.5) * scale, 0.0) for c in range(3)]

    def norms(x, y, z, n, codes):
        i = (x * dy + y) * dz + z
        t = point(x, y, z)
        norm = soft
        for c in range(3):
            d = t[c] - offs[c, :codes]
            norm = norm + d * d
        for k, v in enumerate(parts_of(norm)):
            for block in range(codes // 8):
                v_scr[n, block, 8 * k : 8 * k + 8, :] = v[8 * block : 8 * block + 8]
        if last:
            reach[pl.ds(i, 1), :] = jnp.maximum(jnp.maximum(jnp.abs(t[0]), jnp.abs(t[1])), jnp.abs(t[2]))

    def gather(x, y, z, n, codes, acc, leans):
        i = (x * dy + y) * dz + z
        fixed = t_scr[i]
        for shift in codes:
            code = shifts.index(shift)
            other = ((x + shift[0]) * ey + y + shift[1]) * ez + z + shift[2]
            moved = v_scr[n, code // 8, pl.ds(code % 8, 16, stride=8), :].astype(jnp.bfloat16)
            right = jnp.concatenate([fixed, moved], axis=0)
            v = jnp.dot(a_scr[other], right, preferred_element_type=jnp.float32)
            r = lax.rsqrt(v)
            g = r * jnp.maximum(top - v, 0.0)
            w = g * g * r
            hi = w.astype(jnp.bfloat16)
            lo = (w - hi.astype(jnp.float32)).astype(jnp.bfloat16)
            f = jnp.dot(
                r_scr[other],
                jnp.concatenate([hi, lo], axis=0),
                preferred_element_type=jnp.float32,
            )
            acc = acc + f
            for c in range(3):
                if shift[c] != 1:
                    leans[c] = leans[c] + f[8:] * float(shift[c] - 1)
        return acc, leans

    def early(shift, x, z):
        return shift[1] == 1 and 0 <= x + shift[0] - 1 < dx and 0 <= z + shift[2] - 1 < dz

    @pl.loop(0, dy)
    def _(y):
        @pl.loop(0, dx // pair)
        def _(half):
            for n in range(pair):
                for z in range(dz):
                    norms(half * pair + n, y, z, (half * pair + n) * dz + z, 16)

        for x in range(dx):
            for z in range(dz):
                codes = [s for s in shifts if early(s, x, z)]
                acc, leans = gather(x, y, z, x * dz + z, codes, jnp.zeros((16, 128), jnp.float32), [zeros] * 3)
                i = (x * dy + y) * dz + z
                p_scr[i, :16] = acc
                p_scr[i, 16:24] = leans[0]
                p_scr[i, 24:] = leans[2]

    for copy in copies:
        copy.wait()

    per = 8 // ez

    @pl.loop(0, ey // per)
    def _(q):
        for side in range(2):
            cells = halo_x[side, pl.ds(q * per, per)]
            prepare(cells, lambda j: (side * (ex - 1) * ey + q * per + j // ez) * ez + j % ez, side, None)

    @pl.loop(0, dx)
    def _(x):
        prepare(halo_y[x], lambda j: ((x + 1) * ey + j // ez * (ey - 1)) * ez + j % ez, 0, None)
        prepare(halo_z[x], lambda j: ((x + 1) * ey + j % dy + 1) * ez + j // dy * (ez - 1), 1, None)

    def three(v, k):
        return v[k : k + 1] + v[k + 1 : k + 2] + v[k + 2 : k + 3]

    def finish(x, y, z, n, like):
        i = (x * dy + y) * dz + z
        norms(x, y, z, n, 32)
        codes = [s for s in shifts if not early(s, like, z)]
        acc, leans = gather(x, y, z, n, codes, p_scr[i, :16], [p_scr[i, 16:24], zeros, p_scr[i, 24:]])
        t = point(x, y, z)
        m = three(acc, 11)
        cell = own[x, y, z]
        for c, k in enumerate((0, 3, 8)):
            pull = gain * (three(acc, k) + scale * three(leans[c], 3) - t[c] * m)
            if last:
                out[c, pl.ds(i, 1), :] = jnp.where(cell[3:] > 0.0, base_in[c, pl.ds(i, 1), :] + pull * (1 / 6), 0.0)
            else:
                moved = cell[c : c + 1] + base_in[c, pl.ds(i, 1), :]
                out[c, pl.ds(i, 1), :] = moved + pull * (1 / 3)
                drift[x, y, z, c : c + 1, :] = moved + 0.5 * pull
        if not last:
            drift[x, y, z, 3:, :] = cell[3:]

    wide = 2 if (dx - 2) % 2 == 0 else 1

    @pl.loop(0, (dx - 2) // wide * dy)
    def _(step):
        for n in range(wide):
            for z in range(dz):
                finish(1 + step // dy * wide + n, step % dy, z, n * dz + z, 1)

    @pl.loop(0, dy)
    def _(y):
        for n, x in enumerate((0, dx - 1)):
            for z in range(dz):
                finish(x, y, z, n * dz + z, x)


def pull_field(cells, base_in, last):
    dx, dy, dz, comps, slots = cells.shape
    dims, sizes = (dx, dy, dz), [lax.axis_size(a) for a in axes]
    own, every = dx * dy * dz, (dx + 2) * (dy + 2) * (dz + 2)
    field = jax.ShapeDtypeStruct((3, own, slots), jnp.float32)
    second = jax.ShapeDtypeStruct((own, slots) if last else cells.shape, jnp.float32)
    halos = [
        jax.ShapeDtypeStruct(s + (comps, slots), jnp.float32)
        for s in ((2, dy + 2, dz + 2), (dx, 2, dz + 2), (dx, 2, dy))
    ]
    vmem = pl.BlockSpec(memory_space=pltpu.VMEM)
    return pl.pallas_call(
        functools.partial(pull_kernel, dims, sizes, last),
        out_shape=[field, second] + halos,
        in_specs=[vmem] * 2,
        out_specs=[vmem] * 5,
        scratch_shapes=[
            pltpu.VMEM((every, slots, K), jnp.bfloat16),
            pltpu.VMEM((every, 16, 2 * slots), jnp.bfloat16),
            pltpu.VMEM((own, 32, slots), jnp.bfloat16),
            pltpu.VMEM((dx * dz, 4, 16 * 8, slots), jnp.float32),
            pltpu.VMEM((own, 32, slots), jnp.float32),
            pltpu.VMEM((3, 32, slots), jnp.float32),
            pltpu.VMEM((2, 32, slots), jnp.float32),
            pltpu.VMEM((2, K * 8, slots), jnp.float32),
            pltpu.VMEM((2, 16 * 8, slots), jnp.float32),
            pltpu.VMEM((2, 32 * 8, slots), jnp.float32),
            pltpu.SemaphoreType.DMA((len(moves),)),
            pltpu.SemaphoreType.DMA((len(moves),)),
        ],
        compiler_params=pltpu.CompilerParams(
            collective_id=int(last),
            has_side_effects=True,
            vmem_limit_bytes=52 * 2**20,
        ),
        name="pulls",
    )(cells, base_in)


def far_kernel(dims, src, part, near, out, w_scr):
    dx, dy, dz = dims
    ey, ez = dy + 2, dz + 2
    out[...] = near[...]

    @pl.loop(0, dx * dy * dz)
    def _(i):
        x, y, z = i // (dy * dz), i // dz % dy, i % dz
        me = src[((x + 1) * ey + y + 1) * ez + z + 1]
        held = me[3:] > 0.0
        t = [jnp.where(held, jnp.abs(me[c : c + 1] - 0.5) * scale, 0.0) for c in range(3)]

        @pl.when(jnp.max(jnp.maximum(jnp.maximum(t[0], t[1]), t[2])) > far)
        def _():
            def one(code, carry):
                sx, sy, sz = code // 9, code // 3 % 3, code % 3
                w_scr[:4, :] = src[((x + sx) * ey + y + sy) * ez + z + sz]
                cols = w_scr[...].T
                deltas = []
                q = 0.0
                for c, s in enumerate((sx, sy, sz)):
                    d = cols[:, c : c + 1] + (s - 1).astype(jnp.float32) - me[c : c + 1]
                    deltas.append(d)
                    q = q + d * d
                r = lax.rsqrt(q + soft_sq)
                taper = jnp.maximum(1.0 - q * (1.0 / cut_sq), 0.0)
                w = cols[:, 3:4] * (r * r * r) * (taper * taper)
                return tuple(
                    v + jnp.sum(w * d, axis=0, keepdims=True) for v, d in zip(carry, deltas)
                )

            zero = jnp.zeros((1, 128), jnp.float32)
            pulls = lax.fori_loop(0, 27, one, (zero, zero, zero))
            for c in range(3):
                out[c, pl.ds(i, 1), :] = jnp.where(held, part[c, pl.ds(i, 1), :] + pulls[c] * (1 / 6), 0.0)


def far_field(cells, part, near, halo_x, halo_y, halo_z):
    dx, dy, dz, comps, slots = cells.shape
    ring = jnp.moveaxis(halo_z, 1, 2)
    inner = jnp.concatenate([ring[:, :, :1], cells, ring[:, :, 1:]], axis=2)
    inner = jnp.concatenate([halo_y[:, :1], inner, halo_y[:, 1:]], axis=1)
    every = jnp.concatenate([halo_x[:1], inner, halo_x[1:]], axis=0)
    vmem = pl.BlockSpec(memory_space=pltpu.VMEM)
    return pl.pallas_call(
        functools.partial(far_kernel, (dx, dy, dz)),
        out_shape=jax.ShapeDtypeStruct(near.shape, jnp.float32),
        in_specs=[vmem] * 3,
        out_specs=vmem,
        scratch_shapes=[pltpu.VMEM((8, slots), jnp.float32)],
        name="far_pulls",
    )(every.reshape(-1, comps, slots), part, near)


def body(halo_position, halo_velocity, halo_mass, cell_counts):
    slots = halo_mass.shape[3]
    occupied = lax.broadcasted_iota(jnp.int32, halo_mass.shape, 3) < cell_counts[..., None]
    held_mass = jnp.where(occupied, halo_mass, 0.0)
    cells = jnp.concatenate([jnp.moveaxis(halo_position, 0, 3), held_mass[..., None, :]], axis=3)
    part, drift = pull_field(cells, halo_velocity.reshape(3, -1, slots), False)[:2]
    near, reach, *halos = pull_field(drift, part, True)
    predicted = lax.cond(
        jnp.max(reach) > far,
        lambda: far_field(drift, part, near, *halos),
        lambda: near,
    )
    return predicted.reshape(halo_position.shape)


def solution(mesh):
    return jax.shard_map(
        body,
        mesh=mesh,
        in_specs=(
            P(None, "gx", "gy", "gz", None),
            P(None, "gx", "gy", "gz", None),
            P("gx", "gy", "gz", None),
            P("gx", "gy", "gz"),
        ),
        out_specs=P(None, "gx", "gy", "gz", None),
        check_vma=False,
    )
```

```python
import functools
import itertools

import jax
import jax.numpy as jnp
from jax import lax
from jax.experimental import pallas as pl
from jax.experimental.pallas import tpu as pltpu
from jax.sharding import PartitionSpec as P

soft_sq = 0.01
cut_sq = 0.64
scale = 1.25
soft = soft_sq * scale * scale
top = 1.0 + soft
gain = scale**3 / scale
far = 8.0
K = 48


axes = ("gx", "gy", "gz")
MESH = pl.DeviceIdType.MESH
moves = sorted((o for o in itertools.product((-1, 0, 1), repeat=3) if any(o)), key=lambda o: -sum(map(abs, o)))
shifts = sorted(itertools.product(range(3), repeat=3), key=lambda s: s[1] != 1)


def parts_of(value):
    first = value.astype(jnp.bfloat16).astype(jnp.float32)
    rest = value - first
    second = rest.astype(jnp.bfloat16).astype(jnp.float32)
    third = (rest - second).astype(jnp.bfloat16).astype(jnp.float32)
    return first, second, third


def neighbours(sizes):
    me = [lax.axis_index(a) for a in axes]
    near = [(m, lax.rem(m + 1, n), lax.rem(m + n - 1, n)) for m, n in zip(me, sizes)]
    return {move: tuple(v[o] for v, o in zip(near, move)) for move in moves}


def halo_copies(dims, there, own, halo_x, halo_y, halo_z, send_sem, recv_sem):
    def leaving(o, d):
        return pl.ds(0, d) if o == 0 else pl.ds(d - 1 if o > 0 else 0, 1)

    def landing(o, d):
        return pl.ds(1, d) if o == 0 else pl.ds(0 if o > 0 else d + 1, 1)

    copies = []
    for code, move in enumerate(moves):
        ox, oy, oz = move
        side = [0 if o > 0 else 1 for o in move]
        edge = [d - 1 if o > 0 else 0 for o, d in zip(move, dims)]
        ys, zs = leaving(oy, dims[1]), leaving(oz, dims[2])
        if ox:
            src = own.at[edge[0], ys, zs]
            dst = halo_x.at[side[0], landing(oy, dims[1]), landing(oz, dims[2])]
        elif oy:
            src = own.at[:, edge[1], zs]
            dst = halo_y.at[:, side[1], landing(oz, dims[2])]
        else:
            src = own.at[:, :, edge[2]]
            dst = halo_z.at[:, side[2]]
        copies.append(
            pltpu.make_async_remote_copy(
                src_ref=src,
                dst_ref=dst,
                send_sem=send_sem.at[code],
                recv_sem=recv_sem.at[code],
                device_id=there[move],
                device_id_type=MESH,
            )
        )
    return copies


def pull_kernel(dims, sizes, last, *refs):
    if last:
        own, base_in, out, reach, halo_x, halo_y, halo_z, *scratch = refs
        drift = None
    else:
        position, mass_in, base_in, out, drift, own, halo_x, halo_y, halo_z, *scratch = refs
    a_scr, r_scr, t_scr, v_scr, p_scr, offs, raw_scr, row_scr, m_scr, w_scr, send_sem, recv_sem = scratch
    dx, dy, dz = dims
    ex, ey, ez = dx + 2, dy + 2, dz + 2
    barrier = pltpu.get_barrier_semaphore()
    there = neighbours(sizes)
    for move in moves:
        pl.semaphore_signal(barrier, inc=1, device_id=there[move], device_id_type=MESH)

    zeros = jnp.zeros((8, 128), jnp.float32)
    if not last:
        for i in range(dx * dy * dz):
            x, y, z = i // (dy * dz), i // dz % dy, i % dz
            for c in range(3):
                own[x, y, z, c : c + 1, :] = position[c, i : i + 1, :]
            own[x, y, z, 3:, :] = mass_in[i : i + 1, :]
    for code, shift in enumerate(shifts):
        for c in range(3):
            offs[c, code : code + 1, :] = jnp.full((1, 128), scale * (shift[c] - 1), jnp.float32)
    for c in range(3):
        offs[c, 27:, :] = jnp.zeros((5, 128), jnp.float32)

    @pl.loop(0, v_scr.shape[0])
    def _(n):
        v_scr[n] = jnp.zeros(v_scr.shape[1:], jnp.float32)
        for c in range(3):
            for k in range(3 + 3 * c, 6 + 3 * c):
                for block in range(4):
                    v_scr[n, block, 8 * k : 8 * k + 8, :] = 2 * offs[c, 8 * block : 8 * block + 8]

    row_scr[...] = jnp.zeros(row_scr.shape, jnp.float32)
    m_scr[...] = jnp.zeros(m_scr.shape, jnp.float32)
    w_scr[...] = jnp.zeros(w_scr.shape, jnp.float32)
    row_scr[:, 256:280, :] = jnp.ones((row_scr.shape[0], 24, 128), jnp.float32)
    w_scr[:, 144:168, :] = jnp.ones((w_scr.shape[0], 24, 128), jnp.float32)

    def prepare(cells, place, slot, targets):
        cells = cells.reshape(8, 4, 128)
        for j in range(8):
            raw_scr[slot, 4 * j : 4 * j + 4, :] = cells[j]
        mass = raw_scr[slot, pl.ds(3, 8, stride=4), :]
        a = [(raw_scr[slot, pl.ds(c, 8, stride=4), :] - 0.5) * scale for c in range(3)]
        a = [jnp.where(mass > 0.0, v, 0.0) for v in a]
        split = [parts_of(v) for v in a]
        norm = parts_of(a[0] * a[0] + a[1] * a[1] + a[2] * a[2])
        left = []
        for p in split:
            left += [p[0], p[0], p[1], p[0], p[2], p[1]]
        left += list(norm) + [None] * 14
        for p in split:
            left += list(p)
        for k, v in enumerate(left):
            if v is not None:
                row_scr[slot, 8 * k : 8 * k + 8, :] = v
        mm = [parts_of(mass * v) for v in a] + [parts_of(mass)]
        order = list(mm[0]) + list(mm[1]) + [None] * 2 + list(mm[2]) + list(mm[3])
        for k, v in enumerate(order):
            if v is not None:
                m_scr[slot, 8 * k : 8 * k + 8, :] = v
        for j in range(8):
            a_scr[place(j)] = row_scr[slot, pl.ds(j, K, stride=8), :].T.astype(jnp.bfloat16)
            r = m_scr[slot, pl.ds(j, 16, stride=8), :].astype(jnp.bfloat16)
            r_scr[place(j)] = jnp.concatenate([r, r], axis=1)
        if targets is not None:
            right = []
            for c in range(3):
                p = parts_of(a[c] * -2.0)
                right += [p[0], p[1], p[0], p[2], p[0], p[1]]
            for k, v in enumerate(right):
                w_scr[slot, 8 * k : 8 * k + 8, :] = v
            for j in range(8):
                t_scr[targets + j] = w_scr[slot, pl.ds(j, 32, stride=8), :].astype(jnp.bfloat16)

    def prepare_own(x, slot):
        prepare(own[x], lambda j: ((x + 1) * ey + j // dz + 1) * ez + j % dz + 1, slot, x * dy * dz)

    pair = 2 if dx % 2 == 0 else 1

    four = 4 if dx % 4 == 0 else 1

    @pl.loop(0, dx // four)
    def _(part):
        for n in range(four):
            prepare_own(part * four + n, n)

    pl.semaphore_wait(barrier, len(moves))
    copies = halo_copies(dims, there, own, halo_x, halo_y, halo_z, send_sem, recv_sem)
    for copy in copies:
        copy.start()

    def point(x, y, z):
        cell = own[x, y, z]
        held = cell[3:] > 0.0
        return [jnp.where(held, (cell[c : c + 1] - 0.5) * scale, 0.0) for c in range(3)]

    def norms(x, y, z, n, codes):
        i = (x * dy + y) * dz + z
        t = point(x, y, z)
        norm = soft
        for c in range(3):
            d = t[c] - offs[c, :codes]
            norm = norm + d * d
        for k, v in enumerate(parts_of(norm)):
            for block in range(codes // 8):
                v_scr[n, block, 8 * k : 8 * k + 8, :] = v[8 * block : 8 * block + 8]
        if last:
            reach[pl.ds(i, 1), :] = jnp.maximum(jnp.maximum(jnp.abs(t[0]), jnp.abs(t[1])), jnp.abs(t[2]))

    def gather(x, y, z, n, codes, acc, leans):
        i = (x * dy + y) * dz + z
        fixed = t_scr[i]
        for shift in codes:
            code = shifts.index(shift)
            other = ((x + shift[0]) * ey + y + shift[1]) * ez + z + shift[2]
            moved = v_scr[n, code // 8, pl.ds(code % 8, 16, stride=8), :].astype(jnp.bfloat16)
            right = jnp.concatenate([fixed, moved], axis=0)
            v = jnp.dot(a_scr[other], right, preferred_element_type=jnp.float32)
            r = lax.rsqrt(v)
            g = r * jnp.maximum(top - v, 0.0)
            w = g * g * r
            hi = w.astype(jnp.bfloat16)
            lo = (w - hi.astype(jnp.float32)).astype(jnp.bfloat16)
            f = jnp.dot(
                r_scr[other],
                jnp.concatenate([hi, lo], axis=0),
                preferred_element_type=jnp.float32,
            )
            acc = acc + f
            for c in range(3):
                if shift[c] != 1:
                    leans[c] = leans[c] + f[8:] * float(shift[c] - 1)
        return acc, leans

    def early(shift, x, z):
        return shift[1] == 1 and 0 <= x + shift[0] - 1 < dx and 0 <= z + shift[2] - 1 < dz

    @pl.loop(0, dy)
    def _(y):
        @pl.loop(0, dx // pair)
        def _(half):
            for n in range(pair):
                for z in range(dz):
                    norms(half * pair + n, y, z, (half * pair + n) * dz + z, 16)

        for x in range(dx):
            for z in range(dz):
                codes = [s for s in shifts if early(s, x, z)]
                acc, leans = gather(x, y, z, x * dz + z, codes, jnp.zeros((16, 128), jnp.float32), [zeros] * 3)
                i = (x * dy + y) * dz + z
                p_scr[i, :16] = acc
                p_scr[i, 16:24] = leans[0]
                p_scr[i, 24:] = leans[2]

    for copy in copies:
        copy.wait()

    per = 8 // ez

    for q in range(ey // per):
        for side in range(2):
            cells = halo_x[side, q * per : q * per + per]
            prepare(cells, lambda j: (side * (ex - 1) * ey + q * per + j // ez) * ez + j % ez, (2 * q + side) % 6, None)

    @pl.loop(0, dx // pair)
    def _(half):
        for n in range(pair):
            x = half * pair + n
            prepare(halo_y[x], lambda j: ((x + 1) * ey + j // ez * (ey - 1)) * ez + j % ez, 2 * n, None)
            prepare(halo_z[x], lambda j: ((x + 1) * ey + j % dy + 1) * ez + j // dy * (ez - 1), 2 * n + 1, None)

    def three(v, k):
        return v[k : k + 1] + v[k + 1 : k + 2] + v[k + 2 : k + 3]

    def finish(x, y, z, n):
        i = (x * dy + y) * dz + z
        norms(x, y, z, n, 32)
        codes = [s for s in shifts if not early(s, x, z)]
        acc, leans = gather(x, y, z, n, codes, p_scr[i, :16], [p_scr[i, 16:24], zeros, p_scr[i, 24:]])
        t = point(x, y, z)
        m = three(acc, 11)
        cell = own[x, y, z]
        for c, k in enumerate((0, 3, 8)):
            pull = gain * (three(acc, k) + scale * three(leans[c], 3) - t[c] * m)
            if last:
                out[c, pl.ds(i, 1), :] = jnp.where(cell[3:] > 0.0, base_in[c, pl.ds(i, 1), :] + pull * (1 / 6), 0.0)
            else:
                moved = cell[c : c + 1] + base_in[c, pl.ds(i, 1), :]
                out[c, pl.ds(i, 1), :] = moved + pull * (1 / 3)
                drift[x, y, z, c : c + 1, :] = moved + 0.5 * pull
        if not last:
            drift[x, y, z, 3:, :] = cell[3:]

    @pl.loop(0, dy)
    def _(y):
        for x in range(dx):
            for z in range(dz):
                finish(x, y, z, x * dz + z)


def pull_field(dims, slots, last, *operands):
    dx, dy, dz = dims
    sizes, comps = [lax.axis_size(a) for a in axes], 4
    own, every = dx * dy * dz, (dx + 2) * (dy + 2) * (dz + 2)
    cells = jax.ShapeDtypeStruct((dx, dy, dz, comps, slots), jnp.float32)
    field = jax.ShapeDtypeStruct((3, own, slots), jnp.float32)
    second = jax.ShapeDtypeStruct((own, slots), jnp.float32) if last else cells
    halos = [
        jax.ShapeDtypeStruct(s + (comps, slots), jnp.float32)
        for s in ((2, dy + 2, dz + 2), (dx, 2, dz + 2), (dx, 2, dy))
    ]
    vmem = pl.BlockSpec(memory_space=pltpu.VMEM)
    return pl.pallas_call(
        functools.partial(pull_kernel, dims, sizes, last),
        out_shape=[field, second] + (halos if last else []),
        in_specs=[vmem] * len(operands),
        out_specs=[vmem] * (5 if last else 2),
        scratch_shapes=([] if last else [pltpu.VMEM(h.shape, jnp.float32) for h in [cells] + halos])
        + [
            pltpu.VMEM((every, slots, K), jnp.bfloat16),
            pltpu.VMEM((every, 16, 2 * slots), jnp.bfloat16),
            pltpu.VMEM((own, 32, slots), jnp.bfloat16),
            pltpu.VMEM((dx * dz, 4, 16 * 8, slots), jnp.float32),
            pltpu.VMEM((own, 32, slots), jnp.float32),
            pltpu.VMEM((3, 32, slots), jnp.float32),
            pltpu.VMEM((6, 32, slots), jnp.float32),
            pltpu.VMEM((6, K * 8, slots), jnp.float32),
            pltpu.VMEM((6, 16 * 8, slots), jnp.float32),
            pltpu.VMEM((4, 32 * 8, slots), jnp.float32),
            pltpu.SemaphoreType.DMA((len(moves),)),
            pltpu.SemaphoreType.DMA((len(moves),)),
        ],
        compiler_params=pltpu.CompilerParams(
            collective_id=int(last),
            has_side_effects=True,
            vmem_limit_bytes=52 * 2**20,
        ),
        name="pulls",
    )(*operands)


def far_kernel(dims, reach, own, part, near, halo_x, halo_y, halo_z, out, src, w_scr):
    dx, dy, dz = dims
    ex, ey, ez = dx + 2, dy + 2, dz + 2
    out[...] = near[...]

    @pl.when(jnp.max(reach[...]) > far)
    def _():
        @pl.loop(0, ey)
        def _(y):
            for side in range(2):
                for z in range(ez):
                    src[(side * (ex - 1) * ey + y) * ez + z] = halo_x[side, y, z]

        @pl.loop(0, dx)
        def _(x):
            for side in range(2):
                for z in range(ez):
                    src[((x + 1) * ey + side * (ey - 1)) * ez + z] = halo_y[x, side, z]
                for y in range(dy):
                    src[((x + 1) * ey + y + 1) * ez + side * (ez - 1)] = halo_z[x, side, y]
            for y in range(dy):
                for z in range(dz):
                    src[((x + 1) * ey + y + 1) * ez + z + 1] = own[x, y, z]

        w_scr[...] = jnp.zeros(w_scr.shape, jnp.float32)

        @pl.loop(0, dx * dy * dz)
        def _(i):
            x, y, z = i // (dy * dz), i // dz % dy, i % dz
            me = src[((x + 1) * ey + y + 1) * ez + z + 1]

            @pl.when(jnp.max(reach[pl.ds(i, 1), :]) > far)
            def _():
                def one(code, carry):
                    sx, sy, sz = code // 9, code // 3 % 3, code % 3
                    w_scr[:4, :] = src[((x + sx) * ey + y + sy) * ez + z + sz]
                    cols = w_scr[...].T
                    deltas = []
                    q = 0.0
                    for c, s in enumerate((sx, sy, sz)):
                        d = cols[:, c : c + 1] + (s - 1).astype(jnp.float32) - me[c : c + 1]
                        deltas.append(d)
                        q = q + d * d
                    r = lax.rsqrt(q + soft_sq)
                    taper = jnp.maximum(1.0 - q * (1.0 / cut_sq), 0.0)
                    w = cols[:, 3:4] * (r * r * r) * (taper * taper)
                    return tuple(
                        v + jnp.sum(w * d, axis=0, keepdims=True) for v, d in zip(carry, deltas)
                    )

                zero = jnp.zeros((1, 128), jnp.float32)
                pulls = lax.fori_loop(0, 27, one, (zero, zero, zero))
                for c in range(3):
                    moved = part[c, pl.ds(i, 1), :] + pulls[c] * (1 / 6)
                    out[c, pl.ds(i, 1), :] = jnp.where(me[3:] > 0.0, moved, 0.0)


def far_field(dims, slots, *operands):
    dx, dy, dz = dims
    vmem = pl.BlockSpec(memory_space=pltpu.VMEM)
    every = (dx + 2) * (dy + 2) * (dz + 2)
    return pl.pallas_call(
        functools.partial(far_kernel, dims),
        out_shape=jax.ShapeDtypeStruct((3, dx * dy * dz, slots), jnp.float32),
        in_specs=[vmem] * len(operands),
        out_specs=vmem,
        scratch_shapes=[pltpu.VMEM((every, 4, slots), jnp.float32), pltpu.VMEM((8, slots), jnp.float32)],
        compiler_params=pltpu.CompilerParams(vmem_limit_bytes=8 * 2**20),
        name="far_pulls",
    )(*operands)


def body(halo_position, halo_velocity, halo_mass, cell_counts):
    dims, slots = halo_mass.shape[:3], halo_mass.shape[3]
    occupied = lax.broadcasted_iota(jnp.int32, halo_mass.shape, 3) < cell_counts[..., None]
    mass = jnp.where(occupied, halo_mass, 0.0).reshape(-1, slots)
    position, velocity = (v.reshape(3, -1, slots) for v in (halo_position, halo_velocity))
    part, drift = pull_field(dims, slots, False, position, mass, velocity)
    near, reach, *halos = pull_field(dims, slots, True, drift, part)
    predicted = far_field(dims, slots, reach, drift, part, near, *halos)
    return predicted.reshape(halo_position.shape)


def solution(mesh):
    return jax.shard_map(
        body,
        mesh=mesh,
        in_specs=(
            P(None, "gx", "gy", "gz", None),
            P(None, "gx", "gy", "gz", None),
            P("gx", "gy", "gz", None),
            P("gx", "gy", "gz"),
        ),
        out_specs=P(None, "gx", "gy", "gz", None),
        check_vma=False,
    )
```

```python
import functools
import itertools

import jax
import jax.numpy as jnp
from jax import lax
from jax.experimental import pallas as pl
from jax.experimental.pallas import tpu as pltpu
from jax.sharding import PartitionSpec as P

soft_sq = 0.01
cut_sq = 0.64
scale = 1.25
soft = soft_sq * scale * scale
top = 1.0 + soft
gain = scale**3 / scale
far = 8.0
K = 48


axes = ("gx", "gy", "gz")
MESH = pl.DeviceIdType.MESH
moves = sorted((o for o in itertools.product((-1, 0, 1), repeat=3) if any(o)), key=lambda o: -sum(map(abs, o)))
shifts = sorted(itertools.product(range(3), repeat=3), key=lambda s: s[1] != 1)


def parts_of(value):
    first = value.astype(jnp.bfloat16).astype(jnp.float32)
    rest = value - first
    second = rest.astype(jnp.bfloat16).astype(jnp.float32)
    third = (rest - second).astype(jnp.bfloat16).astype(jnp.float32)
    return first, second, third


def neighbours(sizes):
    me = [lax.axis_index(a) for a in axes]
    near = [(m, lax.rem(m + 1, n), lax.rem(m + n - 1, n)) for m, n in zip(me, sizes)]
    return {move: tuple(v[o] for v, o in zip(near, move)) for move in moves}


def halo_copies(dims, there, own, halo_x, halo_y, halo_z, send_sem, recv_sem):
    def leaving(o, d):
        return pl.ds(0, d) if o == 0 else pl.ds(d - 1 if o > 0 else 0, 1)

    def landing(o, d):
        return pl.ds(1, d) if o == 0 else pl.ds(0 if o > 0 else d + 1, 1)

    copies = []
    for code, move in enumerate(moves):
        ox, oy, oz = move
        side = [0 if o > 0 else 1 for o in move]
        edge = [d - 1 if o > 0 else 0 for o, d in zip(move, dims)]
        ys, zs = leaving(oy, dims[1]), leaving(oz, dims[2])
        if ox:
            src = own.at[edge[0], ys, zs]
            dst = halo_x.at[side[0], landing(oy, dims[1]), landing(oz, dims[2])]
        elif oy:
            src = own.at[:, edge[1], zs]
            dst = halo_y.at[:, side[1], landing(oz, dims[2])]
        else:
            src = own.at[:, :, edge[2]]
            dst = halo_z.at[:, side[2]]
        copies.append(
            pltpu.make_async_remote_copy(
                src_ref=src,
                dst_ref=dst,
                send_sem=send_sem.at[code],
                recv_sem=recv_sem.at[code],
                device_id=there[move],
                device_id_type=MESH,
            )
        )
    return copies


def pull_kernel(dims, sizes, last, *refs):
    if last:
        own, out, reach, halo_x, halo_y, halo_z, *scratch = refs
        drift = None
    else:
        given, (out, drift, position, mass_in, counts, base_in, fetch_sem, own, halo_x, halo_y, halo_z, *scratch) = refs[:4], refs[4:]
    a_scr, r_scr, t_scr, v_scr, p_scr, offs, raw_scr, row_scr, m_scr, w_scr, send_sem, recv_sem = scratch
    dx, dy, dz = dims
    ex, ey, ez = dx + 2, dy + 2, dz + 2
    if not last:
        fetches = [
            pltpu.make_async_copy(src, dst, fetch_sem.at[k])
            for k, (src, dst) in enumerate(zip(given, (position, mass_in, counts, base_in)))
        ]
        for fetch in fetches:
            fetch.start()
    barrier = pltpu.get_barrier_semaphore()
    there = neighbours(sizes)
    for move in moves:
        pl.semaphore_signal(barrier, inc=1, device_id=there[move], device_id_type=MESH)

    zeros = jnp.zeros((8, 128), jnp.float32)
    for code, shift in enumerate(shifts):
        for c in range(3):
            offs[c, code : code + 1, :] = jnp.full((1, 128), scale * (shift[c] - 1), jnp.float32)
    for c in range(3):
        offs[c, 27:, :] = jnp.zeros((5, 128), jnp.float32)

    @pl.loop(0, v_scr.shape[0])
    def _(n):
        v_scr[n] = jnp.zeros(v_scr.shape[1:], jnp.float32)
        for c in range(3):
            for k in range(3 + 3 * c, 6 + 3 * c):
                for block in range(4):
                    v_scr[n, block, 8 * k : 8 * k + 8, :] = 2 * offs[c, 8 * block : 8 * block + 8]

    row_scr[...] = jnp.zeros(row_scr.shape, jnp.float32)
    m_scr[...] = jnp.zeros(m_scr.shape, jnp.float32)
    w_scr[...] = jnp.zeros(w_scr.shape, jnp.float32)
    row_scr[:, 256:280, :] = jnp.ones((row_scr.shape[0], 24, 128), jnp.float32)
    w_scr[:, 144:168, :] = jnp.ones((w_scr.shape[0], 24, 128), jnp.float32)

    if not last:
        for fetch in fetches[:3]:
            fetch.wait()
        lane = lax.broadcasted_iota(jnp.int32, (1, 128), 1)
        for i in range(dx * dy * dz):
            x, y, z = i // (dy * dz), i // dz % dy, i % dz
            for c in range(3):
                own[x, y, z, c : c + 1, :] = position[c, i : i + 1, :]
            held = lane < counts[y, z : z + 1, x : x + 1]
            own[x, y, z, 3:, :] = jnp.where(held, mass_in[i : i + 1, :], 0.0)

    def prepare(cells, place, slot, targets):
        cells = cells.reshape(8, 4, 128)
        for j in range(8):
            raw_scr[slot, 4 * j : 4 * j + 4, :] = cells[j]
        mass = raw_scr[slot, pl.ds(3, 8, stride=4), :]
        a = [(raw_scr[slot, pl.ds(c, 8, stride=4), :] - 0.5) * scale for c in range(3)]
        a = [jnp.where(mass > 0.0, v, 0.0) for v in a]
        split = [parts_of(v) for v in a]
        norm = parts_of(a[0] * a[0] + a[1] * a[1] + a[2] * a[2])
        left = []
        for p in split:
            left += [p[0], p[0], p[1], p[0], p[2], p[1]]
        left += list(norm) + [None] * 14
        for p in split:
            left += list(p)
        for k, v in enumerate(left):
            if v is not None:
                row_scr[slot, 8 * k : 8 * k + 8, :] = v
        mm = [parts_of(mass * v) for v in a] + [parts_of(mass)]
        order = list(mm[0]) + list(mm[1]) + [None] * 2 + list(mm[2]) + list(mm[3])
        for k, v in enumerate(order):
            if v is not None:
                m_scr[slot, 8 * k : 8 * k + 8, :] = v
        for j in range(8):
            a_scr[place(j)] = row_scr[slot, pl.ds(j, K, stride=8), :].T.astype(jnp.bfloat16)
            r = m_scr[slot, pl.ds(j, 16, stride=8), :].astype(jnp.bfloat16)
            r_scr[place(j)] = jnp.concatenate([r, r], axis=1)
        if targets is not None:
            right = []
            for c in range(3):
                p = parts_of(a[c] * -2.0)
                right += [p[0], p[1], p[0], p[2], p[0], p[1]]
            for k, v in enumerate(right):
                w_scr[slot, 8 * k : 8 * k + 8, :] = v
            for j in range(8):
                t_scr[targets + j] = w_scr[slot, pl.ds(j, 32, stride=8), :].astype(jnp.bfloat16)

    def prepare_own(x, slot):
        prepare(own[x], lambda j: ((x + 1) * ey + j // dz + 1) * ez + j % dz + 1, slot, x * dy * dz)

    pair = 2 if dx % 2 == 0 else 1

    four = 4 if dx % 4 == 0 else 1

    @pl.loop(0, dx // four)
    def _(part):
        for n in range(four):
            prepare_own(part * four + n, n)

    pl.semaphore_wait(barrier, len(moves))
    copies = halo_copies(dims, there, own, halo_x, halo_y, halo_z, send_sem, recv_sem)
    for copy in copies:
        copy.start()

    def point(x, y, z):
        cell = own[x, y, z]
        held = cell[3:] > 0.0
        return [jnp.where(held, (cell[c : c + 1] - 0.5) * scale, 0.0) for c in range(3)]

    def norms(x, y, z, n, codes):
        i = (x * dy + y) * dz + z
        t = point(x, y, z)
        norm = soft
        for c in range(3):
            d = t[c] - offs[c, :codes]
            norm = norm + d * d
        for k, v in enumerate(parts_of(norm)):
            for block in range(codes // 8):
                v_scr[n, block, 8 * k : 8 * k + 8, :] = v[8 * block : 8 * block + 8]
        if last:
            size = jnp.maximum(jnp.maximum(jnp.abs(t[0]), jnp.abs(t[1])), jnp.abs(t[2]))
            reach[pl.ds(i, 1), :] = jnp.where(own[x, y, z][3:] > 0.0, size, -1.0)

    def gather(x, y, z, n, codes, acc, leans):
        i = (x * dy + y) * dz + z
        fixed = t_scr[i]
        for shift in codes:
            code = shifts.index(shift)
            other = ((x + shift[0]) * ey + y + shift[1]) * ez + z + shift[2]
            moved = v_scr[n, code // 8, pl.ds(code % 8, 16, stride=8), :].astype(jnp.bfloat16)
            right = jnp.concatenate([fixed, moved], axis=0)
            v = jnp.dot(a_scr[other], right, preferred_element_type=jnp.float32)
            r = lax.rsqrt(v)
            g = r * jnp.maximum(top - v, 0.0)
            w = g * g * r
            hi = w.astype(jnp.bfloat16)
            lo = (w - hi.astype(jnp.float32)).astype(jnp.bfloat16)
            f = jnp.dot(
                r_scr[other],
                jnp.concatenate([hi, lo], axis=0),
                preferred_element_type=jnp.float32,
            )
            acc = acc + f
            for c in range(3):
                if shift[c] != 1:
                    leans[c] = leans[c] + f[8:] * float(shift[c] - 1)
        return acc, leans

    def early(shift, x, z):
        return shift[1] == 1 and 0 <= x + shift[0] - 1 < dx and 0 <= z + shift[2] - 1 < dz

    @pl.loop(0, dy)
    def _(y):
        @pl.loop(0, dx // pair)
        def _(half):
            for n in range(pair):
                for z in range(dz):
                    norms(half * pair + n, y, z, (half * pair + n) * dz + z, 16)

        for x in range(dx):
            for z in range(dz):
                codes = [s for s in shifts if early(s, x, z)]
                acc, leans = gather(x, y, z, x * dz + z, codes, jnp.zeros((16, 128), jnp.float32), [zeros] * 3)
                i = (x * dy + y) * dz + z
                p_scr[i, :16] = acc
                p_scr[i, 16:24] = leans[0]
                p_scr[i, 24:] = leans[2]

    for copy in copies:
        copy.wait()
    if not last:
        fetches[3].wait()

    per = 8 // ez

    for q in range(ey // per):
        for side in range(2):
            cells = halo_x[side, q * per : q * per + per]
            prepare(cells, lambda j: (side * (ex - 1) * ey + q * per + j // ez) * ez + j % ez, (2 * q + side) % 6, None)

    @pl.loop(0, dx // pair)
    def _(half):
        for n in range(pair):
            x = half * pair + n
            prepare(halo_y[x], lambda j: ((x + 1) * ey + j // ez * (ey - 1)) * ez + j % ez, 2 * n, None)
            prepare(halo_z[x], lambda j: ((x + 1) * ey + j % dy + 1) * ez + j // dy * (ez - 1), 2 * n + 1, None)

    def three(v, k):
        return v[k : k + 1] + v[k + 1 : k + 2] + v[k + 2 : k + 3]

    def finish(x, y, z, n):
        i = (x * dy + y) * dz + z
        norms(x, y, z, n, 32)
        codes = [s for s in shifts if not early(s, x, z)]
        acc, leans = gather(x, y, z, n, codes, p_scr[i, :16], [p_scr[i, 16:24], zeros, p_scr[i, 24:]])
        t = point(x, y, z)
        m = three(acc, 11)
        cell = own[x, y, z]
        for c, k in enumerate((0, 3, 8)):
            pull = gain * (three(acc, k) + scale * three(leans[c], 3) - t[c] * m)
            if last:
                out[c, pl.ds(i, 1), :] = pull * (1 / 6)
            else:
                moved = cell[c : c + 1] + base_in[c, pl.ds(i, 1), :]
                out[c, pl.ds(i, 1), :] = moved + pull * (1 / 3)
                drift[x, y, z, c : c + 1, :] = moved + 0.5 * pull
        if not last:
            drift[x, y, z, 3:, :] = cell[3:]

    @pl.loop(0, dy)
    def _(y):
        for x in range(dx):
            for z in range(dz):
                finish(x, y, z, x * dz + z)


def pull_field(dims, slots, last, *operands):
    dx, dy, dz = dims
    sizes, comps = [lax.axis_size(a) for a in axes], 4
    own, every = dx * dy * dz, (dx + 2) * (dy + 2) * (dz + 2)
    cells = jax.ShapeDtypeStruct((dx, dy, dz, comps, slots), jnp.float32)
    field = jax.ShapeDtypeStruct((3, own, slots), jnp.float32)
    second = jax.ShapeDtypeStruct((own, slots), jnp.float32) if last else cells
    halos = [
        jax.ShapeDtypeStruct(s + (comps, slots), jnp.float32)
        for s in ((2, dy + 2, dz + 2), (dx, 2, dz + 2), (dx, 2, dy))
    ]
    vmem = pl.BlockSpec(memory_space=pltpu.VMEM)
    fetched = [pltpu.VMEM(v.shape, v.dtype) for v in operands] + [pltpu.SemaphoreType.DMA((len(operands),))]
    return pl.pallas_call(
        functools.partial(pull_kernel, dims, sizes, last),
        out_shape=[field, second] + (halos if last else []),
        in_specs=[vmem if last else pl.BlockSpec(memory_space=pltpu.HBM)] * len(operands),
        out_specs=[vmem] * (5 if last else 2),
        scratch_shapes=([] if last else fetched + [pltpu.VMEM(h.shape, jnp.float32) for h in [cells] + halos])
        + [
            pltpu.VMEM((every, slots, K), jnp.bfloat16),
            pltpu.VMEM((every, 16, 2 * slots), jnp.bfloat16),
            pltpu.VMEM((own, 32, slots), jnp.bfloat16),
            pltpu.VMEM((dx * dz, 4, 16 * 8, slots), jnp.float32),
            pltpu.VMEM((own, 32, slots), jnp.float32),
            pltpu.VMEM((3, 32, slots), jnp.float32),
            pltpu.VMEM((6, 32, slots), jnp.float32),
            pltpu.VMEM((6, K * 8, slots), jnp.float32),
            pltpu.VMEM((6, 16 * 8, slots), jnp.float32),
            pltpu.VMEM((4, 32 * 8, slots), jnp.float32),
            pltpu.SemaphoreType.DMA((len(moves),)),
            pltpu.SemaphoreType.DMA((len(moves),)),
        ],
        compiler_params=pltpu.CompilerParams(
            collective_id=int(last),
            has_side_effects=True,
            vmem_limit_bytes=52 * 2**20 if last else 66_700_000,
        ),
        name="pulls",
    )(*operands)


def far_kernel(dims, reach, own, part, near, halo_x, halo_y, halo_z, out, src, w_scr):
    dx, dy, dz = dims
    ex, ey, ez = dx + 2, dy + 2, dz + 2
    held = reach[...] >= 0.0
    for c in range(3):
        out[c] = jnp.where(held, part[c] + near[c], 0.0)

    @pl.when(jnp.max(reach[...]) > far)
    def _():
        @pl.loop(0, ey)
        def _(y):
            for side in range(2):
                for z in range(ez):
                    src[(side * (ex - 1) * ey + y) * ez + z] = halo_x[side, y, z]

        @pl.loop(0, dx)
        def _(x):
            for side in range(2):
                for z in range(ez):
                    src[((x + 1) * ey + side * (ey - 1)) * ez + z] = halo_y[x, side, z]
                for y in range(dy):
                    src[((x + 1) * ey + y + 1) * ez + side * (ez - 1)] = halo_z[x, side, y]
            for y in range(dy):
                for z in range(dz):
                    src[((x + 1) * ey + y + 1) * ez + z + 1] = own[x, y, z]

        w_scr[...] = jnp.zeros(w_scr.shape, jnp.float32)

        @pl.loop(0, dx * dy * dz)
        def _(i):
            x, y, z = i // (dy * dz), i // dz % dy, i % dz
            me = src[((x + 1) * ey + y + 1) * ez + z + 1]

            @pl.when(jnp.max(reach[pl.ds(i, 1), :]) > far)
            def _():
                def one(code, carry):
                    sx, sy, sz = code // 9, code // 3 % 3, code % 3
                    w_scr[:4, :] = src[((x + sx) * ey + y + sy) * ez + z + sz]
                    cols = w_scr[...].T
                    deltas = []
                    q = 0.0
                    for c, s in enumerate((sx, sy, sz)):
                        d = cols[:, c : c + 1] + (s - 1).astype(jnp.float32) - me[c : c + 1]
                        deltas.append(d)
                        q = q + d * d
                    r = lax.rsqrt(q + soft_sq)
                    taper = jnp.maximum(1.0 - q * (1.0 / cut_sq), 0.0)
                    w = cols[:, 3:4] * (r * r * r) * (taper * taper)
                    return tuple(
                        v + jnp.sum(w * d, axis=0, keepdims=True) for v, d in zip(carry, deltas)
                    )

                zero = jnp.zeros((1, 128), jnp.float32)
                pulls = lax.fori_loop(0, 27, one, (zero, zero, zero))
                for c in range(3):
                    moved = part[c, pl.ds(i, 1), :] + pulls[c] * (1 / 6)
                    out[c, pl.ds(i, 1), :] = jnp.where(me[3:] > 0.0, moved, 0.0)


def far_field(dims, slots, *operands):
    dx, dy, dz = dims
    vmem = pl.BlockSpec(memory_space=pltpu.VMEM)
    every = (dx + 2) * (dy + 2) * (dz + 2)
    return pl.pallas_call(
        functools.partial(far_kernel, dims),
        out_shape=jax.ShapeDtypeStruct((3, dx * dy * dz, slots), jnp.float32),
        in_specs=[vmem] * len(operands),
        out_specs=vmem,
        scratch_shapes=[pltpu.VMEM((every, 4, slots), jnp.float32), pltpu.VMEM((8, slots), jnp.float32)],
        compiler_params=pltpu.CompilerParams(vmem_limit_bytes=8 * 2**20),
        name="far_pulls",
    )(*operands)


def body(halo_position, halo_velocity, halo_mass, cell_counts):
    dims, slots = halo_mass.shape[:3], halo_mass.shape[3]
    mass, counts = halo_mass.reshape(-1, slots), cell_counts.transpose(1, 2, 0)
    position, velocity = (v.reshape(3, -1, slots) for v in (halo_position, halo_velocity))
    part, drift = pull_field(dims, slots, False, position, mass, counts, velocity)
    near, reach, *halos = pull_field(dims, slots, True, drift)
    predicted = far_field(dims, slots, reach, drift, part, near, *halos)
    return predicted.reshape(halo_position.shape)


def solution(mesh):
    return jax.shard_map(
        body,
        mesh=mesh,
        in_specs=(
            P(None, "gx", "gy", "gz", None),
            P(None, "gx", "gy", "gz", None),
            P("gx", "gy", "gz", None),
            P("gx", "gy", "gz"),
        ),
        out_specs=P(None, "gx", "gy", "gz", None),
        check_vma=False,
    )
```
